32 devices in a mesh: lat: 8 (over z, y), ch: 4 (over x, core).
Axes of the slice: x: 2, y: 2, z: 4, core: 2. Of those that a mesh axis runs over, the one named last changes fastest.
Arguments:
- field: bfloat16 [728, 256, 1440], P('lat', 'ch'), may hold values from -6 to 6
- legendre: bfloat16 [384, 721, 728], P(('lat', 'ch')), may hold values from -0.21875 to 0.21875
- pair_order: int32 [384], replicated, may hold values from 0 to 383, each once
Outputs:
- coeffs: float32 [384, 721, 2, 256], P(('lat', 'ch'))
The draws below stay inside these ranges and needn't reach their ends.
Inputs may be any that keep to these rules, and one draw needn't show every extreme that they name: `pair_order`: each of 0 to 383 appears once; a value p below 360 gives its bin the orders p and 719 - p, and a bin with a larger value is empty.
All inputs are finite; a program needn't handle non-finite values.
Results may differ from the reference program's by a relative error of at most 0.0037.
Values may be sent and summed in bfloat16 or wider, within the bound.
A program may use at most 256 MiB of HBM per device.

```python
import math
import jax
import jax.numpy as jnp
from jax import lax

NLAT = 721
NLON = 1440
C = 256
LMAX = 720
BINS = 384
LATP = 728
N_LAT = 8


def shard_levels(rng, shape, split, low, top_value):
    def one(dim, parts):
        draws = jax.random.uniform(jax.random.fold_in(jax.random.fold_in(rng, 6), dim), (parts,), jnp.float32, low / len(split), top_value / len(split))
        return jnp.repeat(jnp.exp(draws), shape[dim] // parts).reshape((-1,) + (1,) * (len(shape) - dim - 1))

    gain = one(*split[0])
    for cut in split[1:]:
        gain = gain * one(*cut)
    return gain


def noise(key, dims, width, limit, shards=(), held_as=jnp.bfloat16):
    result = width * jax.random.normal(key, dims, jnp.float32)
    if shards:
        result = result * shard_levels(key, dims, shards, -0.22, 0.18)
    return jnp.clip(result, -limit, limit).astype(held_as)


def setup_inputs(seed: int = 0) -> dict:
    keys = jax.random.split(jax.random.key(seed), 4)
    field = noise(keys[0], (LATP, C, NLON), 1.0, 6.0, ((0, 8), (1, 4)))
    legendre = noise(keys[1], (BINS, LMAX + 1, LATP), NLAT ** -0.5, 0.21875, ((0, 32),))
    pair_order = jax.random.permutation(keys[2], BINS).astype(jnp.int32)
    return {"field": field, "legendre": legendre, "pair_order": pair_order}


def dft_table(points, modes, lon_count):
    turns = (points[:, None] * modes[None, :]) % lon_count
    angle = turns.astype(jnp.float32) * (2.0 * math.pi / lon_count)
    return jnp.stack([jnp.cos(angle), -jnp.sin(angle)], axis=-1).astype(jnp.bfloat16)


def reference(field, legendre, pair_order):
    lat_total, chan_count, lon_count = field.shape
    max_order = legendre.shape[1] - 1
    lat_index = jnp.arange(lat_total, dtype=jnp.int32)
    masked = jnp.where((lat_index < NLAT)[:, None, None], field, jnp.zeros_like(field))
    dft_basis = dft_table(jnp.arange(lon_count, dtype=jnp.int32), jnp.arange(max_order, dtype=jnp.int32), lon_count)
    dft_basis = dft_basis.reshape(lon_count, 2 * max_order)
    norm_scale = 2.0 * math.pi / lon_count
    lat_blocks = masked.reshape(N_LAT, lat_total // N_LAT, chan_count, lon_count)

    def transform(lat_block):
        output = jnp.dot(lat_block.reshape(-1, lon_count), dft_basis, preferred_element_type=jnp.float32) * norm_scale
        return output.astype(jnp.bfloat16).reshape(lat_block.shape[0], chan_count, max_order, 2)

    fourier = lax.map(transform, lat_blocks).reshape(lat_total, chan_count, max_order, 2)
    keep_mask = pair_order < max_order // 2
    first_order = jnp.where(keep_mask, pair_order, 0).astype(jnp.int32)
    degree = jnp.arange(max_order + 1, dtype=jnp.int32)

    def one_slot(inputs):
        basis_rows, order_one, alive_flag = inputs
        order_two = (max_order - 1 - order_one).astype(jnp.int32)
        rows_one = lax.dynamic_index_in_dim(fourier, order_one, 2, keepdims=False)
        rows_two = lax.dynamic_index_in_dim(fourier, order_two, 2, keepdims=False)
        prod_one = jnp.dot(basis_rows, rows_one.reshape(lat_total, -1), preferred_element_type=jnp.float32)
        prod_two = jnp.dot(basis_rows, rows_two.reshape(lat_total, -1), preferred_element_type=jnp.float32)
        prod_one = prod_one.reshape(max_order + 1, chan_count, 2)
        prod_two = prod_two.reshape(max_order + 1, chan_count, 2)
        chosen = jnp.where((degree < max_order - order_one)[:, None, None], prod_one, prod_two)
        return jnp.transpose(chosen, (0, 2, 1)) * alive_flag.astype(jnp.float32)

    return lax.map(one_slot, (legendre, first_order, keep_mask))
```

```python
import math

import jax
import jax.numpy as jnp
from jax import lax
from jax.sharding import PartitionSpec as P

NLAT = 721
GROUPS = 4


def dft_table(points, modes, lon_count):
    columns = jnp.repeat(modes, 2)
    phase = jnp.tile(jnp.array([0, lon_count // 4], jnp.int32), modes.shape[0])
    turns = (points[:, None] * columns[None, :] + phase[None, :]) % lon_count
    angle = turns.astype(jnp.float32) * (2.0 * math.pi / lon_count)
    return jnp.cos(angle).astype(jnp.bfloat16)


def per_device(field, legendre, pair_order):
    lat_rows, chan_dev, lon_count = field.shape
    own, row_count, _ = legendre.shape
    lat_count = lax.axis_size("lat")
    ch_count = lax.axis_size("ch")
    dev_count = lat_count * ch_count
    me = lax.axis_index("lat") * ch_count + lax.axis_index("ch")
    max_order = row_count - 1
    keep_all = pair_order < max_order // 2
    first_order = jnp.where(keep_all, pair_order, 0)
    orders = jnp.stack([first_order, max_order - 1 - first_order], axis=1)
    bound_own = lax.dynamic_slice_in_dim(max_order - first_order, me * own, own)
    keep_own = lax.dynamic_slice_in_dim(keep_all, me * own, own)
    rows_global = lax.axis_index("lat") * lat_rows + jnp.arange(lat_rows, dtype=jnp.int32)
    in_grid = (rows_global < NLAT)[:, None, None]
    norm_scale = 2.0 * math.pi / lon_count
    points = jnp.arange(lon_count, dtype=jnp.int32)
    degree = jnp.arange(row_count, dtype=jnp.int32)
    groups = math.gcd(GROUPS, own)
    width = own // groups
    by_dev = orders.reshape(dev_count, own, 2)
    outs = []
    for g in range(groups):
        part = by_dev[:, g * width : (g + 1) * width].reshape(-1)
        basis = dft_table(points, part, lon_count)
        fourier = jnp.einsum("ack,kn->anc", field, basis, preferred_element_type=jnp.float32)
        fourier = jnp.where(in_grid, fourier * norm_scale, 0.0).astype(jnp.bfloat16)
        fourier = fourier.reshape(lat_rows, dev_count * width, 4 * chan_dev)
        got = lax.all_to_all(fourier, ("lat", "ch"), split_axis=1, concat_axis=0, tiled=True)
        got = got.reshape(lat_count, ch_count, lat_rows, width, 4, chan_dev)
        got = got.transpose(3, 0, 2, 4, 1, 5)
        got = got.reshape(width, lat_count * lat_rows, 4 * ch_count * chan_dev)
        products = jnp.einsum(
            "brl,bln->brn", legendre[g * width : (g + 1) * width], got, preferred_element_type=jnp.float32
        )
        bound = bound_own[g * width : (g + 1) * width]
        keep = keep_own[g * width : (g + 1) * width]
        upper = degree[None, :, None] < bound[:, None, None]
        half = products.shape[2] // 2
        chosen = jnp.where(upper, products[:, :, :half], products[:, :, half:])
        chosen = chosen * keep[:, None, None].astype(jnp.float32)
        outs.append(chosen.reshape(width, row_count, 2, half // 2))
    return outs[0] if groups == 1 else jnp.concatenate(outs, axis=0)


def solution(mesh):
    in_specs = (P("lat", "ch", None), P(("lat", "ch"), None, None), P())
    out_specs = P(("lat", "ch"), None, None, None)
    return jax.shard_map(
        per_device, mesh=mesh, in_specs=in_specs, out_specs=out_specs, check_vma=False
    )
```
